32 devices in a mesh: fsdp: 32 (over z, y, x, core).
Axes of the slice: x: 2, y: 2, z: 4, core: 2. Of those that a mesh axis runs over, the one named last changes fastest.
Arguments:
- w_query: float32 [2, 960, 960], P(None, 'fsdp')
- w_key: float32 [2, 960, 320], P(None, 'fsdp')
- w_value: float32 [2, 960, 320], P(None, 'fsdp')
- w_out: float32 [2, 960, 960], P(None, 'fsdp')
- w_gate: float32 [2, 960, 2560], P(None, 'fsdp')
- w_up: float32 [2, 960, 2560], P(None, 'fsdp')
- w_down: float32 [2, 2560, 960], P(None, 'fsdp')
- gain_attn: float32 [2, 960], P(None, 'fsdp')
- gain_mlp: float32 [2, 960], P(None, 'fsdp')
- rope_cos: float32 [128, 32], replicated
- rope_sin: float32 [128, 32], replicated
- x_in: bfloat16 [256, 128, 960], P('fsdp')
- y_cot: bfloat16 [256, 128, 960], P('fsdp')
Outputs:
- output 1: bfloat16 [256, 128, 960], P('fsdp')
- output 2: bfloat16 [256, 128, 960], P('fsdp')
- output 3: float32 [2, 960, 960], P(None, 'fsdp')
- output 4: float32 [2, 960, 320], P(None, 'fsdp')
- output 5: float32 [2, 960, 320], P(None, 'fsdp')
- output 6: float32 [2, 960, 960], P(None, 'fsdp')
- output 7: float32 [2, 960, 2560], P(None, 'fsdp')
- output 8: float32 [2, 960, 2560], P(None, 'fsdp')
- output 9: float32 [2, 2560, 960], P(None, 'fsdp')
- output 10: float32 [2, 960], P(None, 'fsdp')
- output 11: float32 [2, 960], P(None, 'fsdp')
All inputs are finite; a program needn't handle non-finite values.
Results may differ from the reference program's by a relative error of at most 0.02.
Values are sent between devices in bfloat16 or wider.
A program may use at most 1 GiB of HBM per device.

```python
import jax
import jax.numpy as jnp
from jax import lax

MODEL_DIM = 960
FFN_DIM = 2560
HEADS = 15
KV_HEADS = 5
HEAD_DIM = 64
SEQ_LEN = 128
TOTAL_BATCH = 256
LAYERS = 2
NORM_EPS = 1e-5
GROUP_SIZE = HEADS // KV_HEADS
HALF_DIM = HEAD_DIM // 2
Q_WIDTH = HEADS * HEAD_DIM
KV_WIDTH = KV_HEADS * HEAD_DIM


def setup_inputs(seed: int = 0) -> dict:
    key_list = jax.random.split(jax.random.key(seed), 13)

    def draw_weight(rng_key, shape, fan_in):
        return jax.random.normal(rng_key, shape, jnp.float32) * fan_in ** -0.5

    offset = jax.random.randint(key_list[9], (), 0, 4096).astype(jnp.float32)
    jitter = jnp.exp(0.1 * jax.random.normal(key_list[10], (HALF_DIM,), jnp.float32))
    inv_freq = 10000.0 ** (-jnp.arange(HALF_DIM, dtype=jnp.float32) / HALF_DIM) * jitter
    angles = (jnp.arange(SEQ_LEN, dtype=jnp.float32) + offset)[:, None] * inv_freq[None, :]
    tok_shape = (TOTAL_BATCH, SEQ_LEN, MODEL_DIM)
    return {
        "w_query": draw_weight(key_list[0], (LAYERS, MODEL_DIM, Q_WIDTH), MODEL_DIM),
        "w_key": draw_weight(key_list[1], (LAYERS, MODEL_DIM, KV_WIDTH), MODEL_DIM),
        "w_value": draw_weight(key_list[2], (LAYERS, MODEL_DIM, KV_WIDTH), MODEL_DIM),
        "w_out": draw_weight(key_list[3], (LAYERS, Q_WIDTH, MODEL_DIM), Q_WIDTH),
        "w_gate": draw_weight(key_list[4], (LAYERS, MODEL_DIM, FFN_DIM), MODEL_DIM),
        "w_up": draw_weight(key_list[5], (LAYERS, MODEL_DIM, FFN_DIM), MODEL_DIM),
        "w_down": draw_weight(key_list[6], (LAYERS, FFN_DIM, MODEL_DIM), FFN_DIM),
        "gain_attn": 1.0 + 0.2 * jax.random.normal(key_list[7], (LAYERS, MODEL_DIM), jnp.float32),
        "gain_mlp": 1.0 + 0.2 * jax.random.normal(key_list[8], (LAYERS, MODEL_DIM), jnp.float32),
        "rope_cos": jnp.cos(angles),
        "rope_sin": jnp.sin(angles),
        "x_in": jax.random.normal(key_list[11], tok_shape, jnp.float32).astype(jnp.bfloat16),
        "y_cot": jax.random.normal(key_list[12], tok_shape, jnp.float32).astype(jnp.bfloat16),
    }


def rms_norm(values, gain):
    vals32 = values.astype(jnp.float32)
    inv_rms = lax.rsqrt(jnp.mean(vals32 * vals32, axis=-1, keepdims=True) + NORM_EPS)
    return (vals32 * inv_rms * gain.astype(jnp.float32)).astype(jnp.bfloat16)


def apply_rope(heads32, rope_cos, rope_sin):
    first_half = heads32[..., :HALF_DIM]
    second_half = heads32[..., HALF_DIM:]
    cos_b = rope_cos[:, None, :]
    sin_b = rope_sin[:, None, :]
    return jnp.concatenate([first_half * cos_b - second_half * sin_b, second_half * cos_b + first_half * sin_b], axis=-1)


def layer_forward(weights, rope_cos, rope_sin, hidden):
    w_query, w_key, w_value, w_out, w_gate, w_up, w_down, gain_attn, gain_mlp = weights
    normed = rms_norm(hidden, gain_attn)
    q_proj = jnp.dot(normed, w_query, preferred_element_type=jnp.float32).reshape(SEQ_LEN, HEADS, HEAD_DIM)
    q_heads = apply_rope(q_proj, rope_cos, rope_sin).astype(jnp.bfloat16).reshape(SEQ_LEN, KV_HEADS, GROUP_SIZE, HEAD_DIM)
    k_proj = jnp.dot(normed, w_key, preferred_element_type=jnp.float32).reshape(SEQ_LEN, KV_HEADS, HEAD_DIM)
    k_heads = apply_rope(k_proj, rope_cos, rope_sin).astype(jnp.bfloat16)
    v_heads = jnp.dot(normed, w_value, preferred_element_type=jnp.float32).astype(jnp.bfloat16).reshape(SEQ_LEN, KV_HEADS, HEAD_DIM)
    scores = jnp.einsum("qkgd,skd->kgqs", q_heads.astype(jnp.float32), k_heads.astype(jnp.float32)) * HEAD_DIM ** -0.5
    positions = jnp.arange(SEQ_LEN)
    scores = jnp.where(positions[:, None] >= positions[None, :], scores, -1e30)
    attn_probs = jax.nn.softmax(scores, axis=-1).astype(jnp.bfloat16)
    attn_heads = jnp.einsum("kgqs,skd->qkgd", attn_probs.astype(jnp.float32), v_heads.astype(jnp.float32))
    attn_heads = attn_heads.astype(jnp.bfloat16).reshape(SEQ_LEN, Q_WIDTH)
    mid_hidden = (hidden.astype(jnp.float32) + jnp.dot(attn_heads, w_out, preferred_element_type=jnp.float32)).astype(jnp.bfloat16)
    normed_mlp = rms_norm(mid_hidden, gain_mlp)
    gate_pre = jnp.dot(normed_mlp, w_gate, preferred_element_type=jnp.float32)
    up_proj = jnp.dot(normed_mlp, w_up, preferred_element_type=jnp.float32)
    mlp_act = (jax.nn.silu(gate_pre) * up_proj).astype(jnp.bfloat16)
    return (mid_hidden.astype(jnp.float32) + jnp.dot(mlp_act, w_down, preferred_element_type=jnp.float32)).astype(jnp.bfloat16)


def reference(w_query, w_key, w_value, w_out, w_gate, w_up, w_down, gain_attn, gain_mlp, rope_cos, rope_sin, x_in, y_cot):
    masters = (w_query, w_key, w_value, w_out, w_gate, w_up, w_down, gain_attn, gain_mlp)
    params_bf = tuple(master.astype(jnp.bfloat16) for master in masters)

    def stack_forward(params, seq_x):
        def layer_body(hidden, layer_params):
            return layer_forward(layer_params, rope_cos, rope_sin, hidden), None
        return lax.scan(layer_body, seq_x, params)[0]

    def per_sequence(grad_sums, seq_pair):
        seq_x, seq_cot = seq_pair
        seq_y, pullback = jax.vjp(stack_forward, params_bf, seq_x)
        grad_params, grad_x = pullback(seq_cot)
        new_sums = tuple(old_sum + grad_part.astype(jnp.float32) for old_sum, grad_part in zip(grad_sums, grad_params))
        return new_sums, (seq_y, grad_x)

    grad_init = tuple(jnp.zeros(master.shape, jnp.float32) for master in masters)
    grads, outputs = lax.scan(per_sequence, grad_init, (x_in, y_cot))
    return (outputs[0], outputs[1], grads[0], grads[1], grads[2], grads[3], grads[4], grads[5], grads[6], grads[7], grads[8])
```

```python
import jax
import jax.numpy as jnp
from jax import lax
from jax.experimental import pallas as pl
from jax.experimental.pallas import tpu as pltpu
from jax.sharding import PartitionSpec as P

NORM_EPS = 1e-5
MASK_VALUE = -1e30
BF = jnp.bfloat16
F32 = jnp.float32
DEVICES = 32
DIM = 960
ROWS = 30
PAD_ROWS = 32
PAD_DIM = DEVICES * PAD_ROWS
FFN_ROWS = 80
QKV = 1600
QKV_PAD = 1664


def flip(bits):
    return [(i, i ^ bits) for i in range(DEVICES)]


CORE, XAX, YAX = 1, 2, 4


def send(values, bits):
    return lax.ppermute(values, "fsdp", flip(bits))


def block_of(dev):
    core, x_at, y_at, z_at = dev % 2, dev // 2 % 2, dev // 4 % 2, dev // 8
    return ((core * 2 + x_at) * 2 + y_at) * 4 + z_at


def one_hot(target, width):
    return (target[:, None] == lax.broadcasted_iota(jnp.int32, (target.shape[0], width), 1)).astype(BF)


def swap_xy(block):
    return (block & 19) | ((block & 8) >> 1) | ((block & 4) << 1)


def dot(left, right, dims):
    return lax.dot_general(left, right, ((dims[:1], dims[1:]), ((), ())), preferred_element_type=F32)


def mm(left, right):
    return dot(left, right, (1, 0))


def pick(values, index):
    return lax.dynamic_index_in_dim(values, index, 0, keepdims=False)


def rms_forward(values, gain):
    vals32 = values.astype(F32)
    inv_rms = lax.rsqrt(jnp.sum(vals32 * vals32, axis=-1, keepdims=True) * (1.0 / DIM) + NORM_EPS)
    return (vals32 * inv_rms * gain.astype(F32)).astype(BF), inv_rms


def rms_backward(values, inv_rms, gain, grad_normed):
    scaled = values.astype(F32) * inv_rms
    grad_scaled = grad_normed * gain.astype(F32)
    grad_gain = jnp.sum(grad_normed * scaled, axis=0)
    mean = jnp.sum(grad_scaled * scaled, axis=-1, keepdims=True) * (1.0 / DIM)
    return inv_rms * (grad_scaled - scaled * mean), grad_gain


def rotary(heads32, rope_cos, rope_sin, sin_sign):
    half_dim = rope_cos.shape[-1]
    first_half = heads32[..., :half_dim]
    second_half = heads32[..., half_dim:]
    cos_b = rope_cos[None, :, None, :]
    sin_b = sin_sign * rope_sin[None, :, None, :]
    return jnp.concatenate([first_half * cos_b - second_half * sin_b, second_half * cos_b + first_half * sin_b], axis=-1)


def layer_forward(weights, rope_cos, rope_sin, hidden, batch, seq_len):
    w_qkv, w_out, w_gate, w_up, w_down, gain_attn, gain_mlp = weights
    head_dim = 2 * rope_cos.shape[-1]
    num_heads, kv_heads = 15, 5
    normed, inv_attn = rms_forward(hidden, gain_attn)
    qkv = mm(normed, w_qkv)
    q_heads = rotary(qkv[:, :960].reshape(batch, seq_len, num_heads, head_dim), rope_cos, rope_sin, 1.0).astype(BF)
    q_heads = q_heads.reshape(batch, seq_len, kv_heads, 3, head_dim)
    k_heads = rotary(qkv[:, 960:1280].reshape(batch, seq_len, kv_heads, head_dim), rope_cos, rope_sin, 1.0).astype(BF)
    v_heads = qkv[:, 1280:1600].astype(BF).reshape(batch, seq_len, kv_heads, head_dim)
    scores = jnp.einsum("bqkgd,bskd->bkgqs", q_heads, k_heads, preferred_element_type=F32) * head_dim ** -0.5
    positions = jnp.arange(seq_len)
    scores = jnp.where(positions[:, None] >= positions[None, :], scores, MASK_VALUE)
    probs = jax.nn.softmax(scores, axis=-1).astype(BF)
    heads = jnp.einsum("bkgqs,bskd->bqkgd", probs, v_heads, preferred_element_type=F32)
    heads = heads.astype(BF).reshape(batch * seq_len, num_heads * head_dim)
    mid = (hidden.astype(F32) + mm(heads, w_out)).astype(BF)
    normed_mlp, inv_mlp = rms_forward(mid, gain_mlp)
    gate_pre = mm(normed_mlp, w_gate)
    up_proj = mm(normed_mlp, w_up)
    act = (jax.nn.silu(gate_pre) * up_proj).astype(BF)
    out = (mid.astype(F32) + mm(act, w_down)).astype(BF)
    return out, (hidden, inv_attn, normed, q_heads, k_heads, v_heads, probs, heads, mid, inv_mlp, normed_mlp, gate_pre, up_proj, act)


def scatter_wide(left_rel, grad, first, second, extra=None):
    def piece(at):
        rows = slice(at * 256, (at + 1) * 256)
        part = dot(left_rel[:, rows], grad, (0, 0))
        return part if extra is None else part + extra[rows]

    far = send(piece(3), CORE)
    near = send(piece(2), CORE)
    across = send(piece(1) + far, first)
    kept = piece(0) + near + across
    return kept[:128] + send(kept[128:], second)


def scatter_down(act, grad, place):
    core, x_at, y_at, z_at = place
    whole = dot(act, grad, (0, 0)).reshape(4, 640, PAD_DIM)

    def piece(d_core, d_x):
        return pick(whole, (core ^ d_core) * 2 + (x_at ^ d_x))

    far = send(piece(1, 1), CORE)
    near = send(piece(1, 0), CORE)
    across = send(piece(0, 1) + far, XAX)
    kept = (piece(0, 0) + near + across).reshape(2, 4 * FFN_ROWS, PAD_DIM)
    part = pick(kept, y_at) + send(pick(kept, y_at ^ 1), YAX)
    part = part.reshape(4, FFN_ROWS, PAD_DIM)
    return jnp.concatenate([pick(part, z_at ^ step) for step in range(4)])


def scatter_z(part):
    half = part.shape[0] // 2
    part = part[:half] + send(part[half:], 16)
    half = half // 2
    return part[:half] + send(part[half:], 8)


def layer_backward(weights, rope_cos, rope_sin, saved, grad_out, batch, seq_len, place, to_rel, nat_to_rel):
    w_qkv, w_out, w_gate, w_up, w_down, gain_attn, gain_mlp = weights
    (hidden, inv_attn, normed, q_heads, k_heads, v_heads, probs, heads, mid, inv_mlp, normed_mlp, gate_pre, up_proj, act) = saved
    head_dim = 2 * rope_cos.shape[-1]
    num_heads = 15
    tokens = hidden.shape[0]
    rel_x, rel_y = to_rel
    down = scatter_down(act, grad_out, place)
    grad_act = dot(grad_out, w_down, (1, 1))
    gate_sig = jax.nn.sigmoid(gate_pre)
    grad_up = (grad_act * gate_pre * gate_sig).astype(BF)
    grad_gate = (grad_act * up_proj * gate_sig * (1.0 + gate_pre * (1.0 - gate_sig))).astype(BF)
    gate = scatter_wide(mm(normed_mlp, rel_x).astype(BF), grad_gate, XAX, YAX)
    up = scatter_wide(mm(normed_mlp, rel_y).astype(BF), grad_up, YAX, XAX)
    from_gate = dot(grad_gate, w_gate, (1, 1))
    grad_normed_mlp = from_gate + dot(grad_up, w_up, (1, 1))
    grad_mid_norm, grad_gain_mlp = rms_backward(mid, inv_mlp, gain_mlp, grad_normed_mlp)
    grad_mid = grad_out.astype(F32) + grad_mid_norm
    grad_mid_bf = grad_mid.astype(BF)
    out = scatter_wide(mm(heads, nat_to_rel).astype(BF), grad_mid_bf, YAX, XAX)
    grad_attn = dot(grad_mid_bf, w_out, (1, 1)).astype(BF).reshape(batch, seq_len, 5, 3, head_dim)
    grad_v = jnp.einsum("bkgqs,bqkgd->bskd", probs, grad_attn, preferred_element_type=F32)
    grad_v = grad_v.astype(BF).reshape(tokens, -1)
    grad_probs = jnp.einsum("bqkgd,bskd->bkgqs", grad_attn, v_heads, preferred_element_type=F32)
    probs32 = probs.astype(F32)
    grad_scores = probs32 * (grad_probs - jnp.sum(probs32 * grad_probs, axis=-1, keepdims=True)) * head_dim ** -0.5
    grad_scores = grad_scores.astype(BF)
    grad_q = jnp.einsum("bkgqs,bskd->bqkgd", grad_scores, k_heads, preferred_element_type=F32)
    grad_q = rotary(grad_q.reshape(batch, seq_len, num_heads, head_dim), rope_cos, rope_sin, -1.0)
    grad_q = grad_q.astype(BF).reshape(tokens, -1)
    grad_k = jnp.einsum("bkgqs,bqkgd->bskd", grad_scores, q_heads, preferred_element_type=F32)
    grad_k = rotary(grad_k, rope_cos, rope_sin, -1.0).astype(BF).reshape(tokens, -1)
    grad_qkv = jnp.concatenate([grad_q, grad_k, grad_v, jnp.zeros((tokens, QKV_PAD - QKV), BF)], axis=1)
    grad_normed = dot(grad_qkv, w_qkv, (1, 1))
    grad_hidden_norm, grad_gain_attn = rms_backward(hidden, inv_attn, gain_attn, grad_normed)
    grad_hidden = (grad_mid + grad_hidden_norm).astype(BF)
    gains = jnp.stack([grad_gain_attn, grad_gain_mlp])
    gain_rows = lax.dot_general(rel_y.astype(F32), gains, (((0,), (1,)), ((), ())), precision=lax.Precision.HIGHEST, preferred_element_type=F32)
    extra = jnp.pad(gain_rows, ((0, 0), (QKV, QKV_PAD - QKV - 2)))
    qkv = scatter_wide(mm(normed, rel_y).astype(BF), grad_qkv, YAX, XAX, extra)
    down = scatter_z(down)
    mlp = scatter_z(jnp.concatenate([gate, up], axis=1))
    attn = scatter_z(jnp.concatenate([qkv, out], axis=1))
    return grad_hidden, (attn[:, :QKV_PAD], attn[:, QKV_PAD:], mlp[:, :2560], mlp[:, 2560:], down)


def gather_kernel(*refs):
    count = (len(refs) - 3) // 2
    shards, wholes = refs[:count], refs[count:2 * count]
    send_sem, recv_sem, own_sem = refs[2 * count:]
    me = lax.axis_index("fsdp")
    core, x_at, y_at, z_at = me % 2, me // 2 % 2, me // 4 % 2, me // 8
    core_peer = me + 1 - 2 * core
    x_peer = me + 2 - 4 * x_at
    y_peer = me + 4 - 8 * y_at
    z_peers = [(z_at + step) % 4 * 8 + me % 8 for step in (1, 2, 3)]
    barrier = pltpu.get_barrier_semaphore()
    for peer in (core_peer, x_peer, y_peer, *z_peers):
        pl.semaphore_signal(barrier, inc=1, device_id=(peer,), device_id_type=pl.DeviceIdType.MESH)
    pl.semaphore_wait(barrier, 6)

    def copy(index, stage, source, target, peer):
        return pltpu.make_async_remote_copy(src_ref=source, dst_ref=target, send_sem=send_sem.at[index, stage], recv_sem=recv_sem.at[index, stage],
                                            device_id=(peer,), device_id_type=pl.DeviceIdType.MESH)

    def z_copies(index):
        return [copy(index, step, shards[index], wholes[index].at[core, x_at, y_at, z_at], z_peers[step]) for step in range(3)]

    def second(index):
        part = wholes[index].at[core, x_at, y_at]
        return copy(index, 3, part, part, y_peer if index % 5 in (2, 4) else x_peer)

    def third(index):
        if index % 5 in (2, 4):
            part = wholes[index].at[core, x_at]
            return copy(index, 4, part, part, x_peer)
        part = wholes[index].at[core, :, y_at]
        return copy(index, 4, part, part, y_peer)

    def last(index):
        part = wholes[index].at[core]
        return copy(index, 5, part, part, core_peer)

    def own(index):
        return pltpu.make_async_copy(shards[index], wholes[index].at[core, x_at, y_at, z_at], own_sem.at[index])

    for index in range(count):
        own(index).start()
        for one in z_copies(index):
            one.start()
    for index in range(count):
        own(index).wait()
        for one in z_copies(index):
            one.wait()
        second(index).start()
        if index >= 2:
            second(index - 2).wait()
            third(index - 2).start()
        if index >= 5:
            third(index - 5).wait()
            last(index - 5).start()
    for index in (count - 2, count - 1):
        second(index).wait()
        third(index).start()
    for index in range(count - 5, count):
        third(index).wait()
        last(index).start()
    for index in range(count):
        last(index).wait()


def gather_all(shards):
    count = len(shards)
    wholes = pl.pallas_call(
        gather_kernel,
        out_shape=[jax.ShapeDtypeStruct((2, 2, 2, 4) + shard.shape, BF) for shard in shards],
        in_specs=[pl.BlockSpec(memory_space=pltpu.VMEM)] * count,
        out_specs=[pl.BlockSpec(memory_space=pl.ANY)] * count,
        scratch_shapes=[pltpu.SemaphoreType.DMA((count, 6)), pltpu.SemaphoreType.DMA((count, 6)), pltpu.SemaphoreType.DMA((count,))],
        compiler_params=pltpu.CompilerParams(collective_id=0, has_side_effects=True, vmem_limit_bytes=8 * 1024 * 1024),
    )(*shards)
    return [whole.reshape(DEVICES * whole.shape[4], whole.shape[5]) for whole in wholes]


def solution(mesh):
    shard_spec = P(None, "fsdp")
    batch_spec = P("fsdp")

    def local_step(w_query, w_key, w_value, w_out, w_gate, w_up, w_down, gain_attn, gain_mlp, rope_cos, rope_sin, x_in, y_cot):
        me = lax.axis_index("fsdp")
        place = (me % 2, me // 2 % 2, me // 4 % 2, me // 8)
        my_block = block_of(me)
        batch, seq_len, _ = x_in.shape
        tokens = batch * seq_len
        natural = lax.iota(jnp.int32, DIM)
        nat_block, nat_row = block_of(natural // ROWS), natural % ROWS
        spread = one_hot(nat_block * PAD_ROWS + nat_row, PAD_DIM)
        nat_to_rel = one_hot(swap_xy(nat_block ^ my_block) * PAD_ROWS + nat_row, PAD_DIM)
        padded = lax.iota(jnp.int32, PAD_DIM)
        rel_block = (padded // PAD_ROWS) ^ my_block
        rel_x = one_hot(rel_block * PAD_ROWS + padded % PAD_ROWS, PAD_DIM)
        rel_y = one_hot(swap_xy(rel_block) * PAD_ROWS + padded % PAD_ROWS, PAD_DIM)

        def pad_rows(values):
            return jnp.pad(values, ((0, 0), (0, PAD_ROWS - ROWS), (0, 0)))

        def ffn_columns(values):
            return values.reshape(2, ROWS, 4, 2, 2, 2, FFN_ROWS).transpose(0, 1, 5, 4, 3, 2, 6).reshape(2, ROWS, -1)

        sh_qkv = pad_rows(jnp.concatenate([w_query, w_key, w_value, gain_attn[:, :, None], gain_mlp[:, :, None], jnp.zeros((2, ROWS, QKV_PAD - QKV - 2), F32)], axis=2).astype(BF))
        sh_out = pad_rows(mm(w_out.astype(BF).reshape(2 * ROWS, DIM), spread).astype(BF).reshape(2, ROWS, PAD_DIM))
        sh_gate = pad_rows(ffn_columns(w_gate.astype(BF)))
        sh_up = pad_rows(ffn_columns(w_up.astype(BF)))
        sh_down = mm(w_down.astype(BF).reshape(2 * FFN_ROWS, DIM), spread).astype(BF).reshape(2, FFN_ROWS, PAD_DIM)

        hidden = mm(x_in.reshape(tokens, DIM), spread).astype(BF)
        grad_hidden = mm(y_cot.reshape(tokens, DIM), spread).astype(BF)
        saved_layers, layer_weights = [], []
        wholes = gather_all([part[layer] for layer in range(2) for part in (sh_qkv, sh_out, sh_gate, sh_up, sh_down)])
        for layer in range(2):
            full_qkv, full_out, full_gate, full_up, full_down = wholes[5 * layer:5 * layer + 5]
            full_out = mm(spread, full_out).astype(BF)
            weights = (full_qkv, full_out, full_gate, full_up, full_down, full_qkv[:, QKV], full_qkv[:, QKV + 1])
            hidden, saved = layer_forward(weights, rope_cos, rope_sin, hidden, batch, seq_len)
            saved_layers.append(saved)
            layer_weights.append(weights)
        y_out = dot(hidden, spread, (1, 1)).astype(BF).reshape(x_in.shape)
        shards = [None, None]
        for layer in (1, 0):
            grad_hidden, shards[layer] = layer_backward(layer_weights[layer], rope_cos, rope_sin, saved_layers[layer], grad_hidden, batch, seq_len, place, (rel_x, rel_y), nat_to_rel)
        dx_in = dot(grad_hidden, spread, (1, 1)).astype(BF).reshape(x_in.shape)

        g_qkv, g_out, g_gate, g_up, g_down = (jnp.stack(pair) for pair in zip(*shards))

        def natural_columns(values, rows):
            flat = values.reshape(2 * values.shape[1], PAD_DIM)
            flat = lax.dot_general(flat, spread.astype(F32), (((1,), (1,)), ((), ())), precision=lax.Precision.HIGHEST, preferred_element_type=F32)
            return flat.reshape(2, values.shape[1], DIM)[:, :rows]

        def natural_ffn(values):
            return values[:, :ROWS].reshape(2, ROWS, 2, 2, 2, 4, FFN_ROWS).transpose(0, 1, 5, 4, 3, 2, 6).reshape(2, ROWS, -1)

        g_qkv = g_qkv[:, :ROWS]
        return (y_out, dx_in, g_qkv[:, :, :960], g_qkv[:, :, 960:1280], g_qkv[:, :, 1280:1600], natural_columns(g_out, ROWS),
                natural_ffn(g_gate), natural_ffn(g_up), natural_columns(g_down, FFN_ROWS), g_qkv[:, :, QKV], g_qkv[:, :, QKV + 1])

    in_specs = (shard_spec,) * 9 + (P(), P(), batch_spec, batch_spec)
    out_specs = (batch_spec, batch_spec) + (shard_spec,) * 9
    return jax.shard_map(local_step, mesh=mesh, in_specs=in_specs, out_specs=out_specs, check_vma=False)
```

```python
import jax
import jax.numpy as jnp
from jax import lax
from jax.experimental import pallas as pl
from jax.experimental.pallas import tpu as pltpu
from jax.sharding import PartitionSpec as P

NORM_EPS = 1e-5
MASK_VALUE = -1e30
BF = jnp.bfloat16
F32 = jnp.float32
DEVICES = 32
DIM = 960
ROWS = 30
PAD_ROWS = 32
PAD_DIM = DEVICES * PAD_ROWS
FFN_ROWS = 80
QKV = 1600
QKV_PAD = 1664


def flip(bits):
    return [(i, i ^ bits) for i in range(DEVICES)]


CORE, XAX, YAX = 1, 2, 4


def send(values, bits):
    return lax.ppermute(values, "fsdp", flip(bits))


def block_of(dev):
    core, x_at, y_at, z_at = dev % 2, dev // 2 % 2, dev // 4 % 2, dev // 8
    return ((core * 2 + x_at) * 2 + y_at) * 4 + z_at


def one_hot(target, width):
    return (target[:, None] == lax.broadcasted_iota(jnp.int32, (target.shape[0], width), 1)).astype(BF)


def swap_xy(block):
    return (block & 19) | ((block & 8) >> 1) | ((block & 4) << 1)


def dot(left, right, dims):
    return lax.dot_general(left, right, ((dims[:1], dims[1:]), ((), ())), preferred_element_type=F32)


def mm(left, right):
    return dot(left, right, (1, 0))


def pick(values, index):
    return lax.dynamic_index_in_dim(values, index, 0, keepdims=False)


def rms_forward(values, gain):
    vals32 = values.astype(F32)
    inv_rms = lax.rsqrt(jnp.sum(vals32 * vals32, axis=-1, keepdims=True) * (1.0 / DIM) + NORM_EPS)
    return (vals32 * inv_rms * gain.astype(F32)).astype(BF), inv_rms


def rms_backward(values, inv_rms, gain, grad_normed):
    scaled = values.astype(F32) * inv_rms
    grad_scaled = grad_normed * gain.astype(F32)
    grad_gain = jnp.sum(grad_normed * scaled, axis=0)
    mean = jnp.sum(grad_scaled * scaled, axis=-1, keepdims=True) * (1.0 / DIM)
    return inv_rms * (grad_scaled - scaled * mean), grad_gain


def rotary(heads32, rope_cos, rope_sin, sin_sign):
    half_dim = rope_cos.shape[-1]
    first_half = heads32[..., :half_dim]
    second_half = heads32[..., half_dim:]
    cos_b = rope_cos[None, :, None, :]
    sin_b = sin_sign * rope_sin[None, :, None, :]
    return jnp.concatenate([first_half * cos_b - second_half * sin_b, second_half * cos_b + first_half * sin_b], axis=-1)


def layer_forward(weights, rope_cos, rope_sin, hidden, batch, seq_len):
    w_qkv, w_out, w_gate, w_up, w_down, gain_attn, gain_mlp = weights
    head_dim = 2 * rope_cos.shape[-1]
    num_heads, kv_heads = 15, 5
    normed, inv_attn = rms_forward(hidden, gain_attn)
    qkv = mm(normed, w_qkv)
    q_heads = rotary(qkv[:, :960].reshape(batch, seq_len, num_heads, head_dim), rope_cos, rope_sin, 1.0).astype(BF)
    q_heads = q_heads.reshape(batch, seq_len, kv_heads, 3, head_dim)
    k_heads = rotary(qkv[:, 960:1280].reshape(batch, seq_len, kv_heads, head_dim), rope_cos, rope_sin, 1.0).astype(BF)
    v_heads = qkv[:, 1280:1600].astype(BF).reshape(batch, seq_len, kv_heads, head_dim)
    scores = jnp.einsum("bqkgd,bskd->bkgqs", q_heads, k_heads, preferred_element_type=F32) * head_dim ** -0.5
    positions = jnp.arange(seq_len)
    scores = jnp.where(positions[:, None] >= positions[None, :], scores, MASK_VALUE)
    probs = jax.nn.softmax(scores, axis=-1).astype(BF)
    heads = jnp.einsum("bkgqs,bskd->bqkgd", probs, v_heads, preferred_element_type=F32)
    heads = heads.astype(BF).reshape(batch * seq_len, num_heads * head_dim)
    mid = (hidden.astype(F32) + mm(heads, w_out)).astype(BF)
    normed_mlp, inv_mlp = rms_forward(mid, gain_mlp)
    gate_pre = mm(normed_mlp, w_gate)
    up_proj = mm(normed_mlp, w_up)
    act = (jax.nn.silu(gate_pre) * up_proj).astype(BF)
    out = (mid.astype(F32) + mm(act, w_down)).astype(BF)
    return out, (hidden, inv_attn, normed, q_heads, k_heads, v_heads, probs, heads, mid, inv_mlp, normed_mlp, gate_pre, up_proj, act)


def scatter_wide(left_rel, grad, first, second, extra=None):
    def piece(at):
        rows = slice(at * 256, (at + 1) * 256)
        part = dot(left_rel[:, rows], grad, (0, 0))
        return part if extra is None else part + extra[rows]

    far = send(piece(3), CORE)
    near = send(piece(2), CORE)
    across = send(piece(1) + far, first)
    kept = piece(0) + near + across
    return kept[:128] + send(kept[128:], second)


def scatter_down(act, grad, place):
    core, x_at, y_at, z_at = place
    whole = dot(act, grad, (0, 0)).reshape(4, 640, PAD_DIM)

    def piece(d_core, d_x):
        return pick(whole, (core ^ d_core) * 2 + (x_at ^ d_x))

    far = send(piece(1, 1), CORE)
    near = send(piece(1, 0), CORE)
    across = send(piece(0, 1) + far, XAX)
    kept = (piece(0, 0) + near + across).reshape(2, 4 * FFN_ROWS, PAD_DIM)
    part = pick(kept, y_at) + send(pick(kept, y_at ^ 1), YAX)
    part = part.reshape(4, FFN_ROWS, PAD_DIM)
    return jnp.concatenate([pick(part, z_at ^ step) for step in range(4)])


def scatter_z(part):
    rows = part.shape[0] // 4
    blocks = [part[step * rows:(step + 1) * rows] for step in range(4)]
    got = send(jnp.concatenate([blocks[1], blocks[3]]), 8)
    return blocks[0] + got[:rows] + send(blocks[2] + got[rows:], 16)


def layer_backward(weights, rope_cos, rope_sin, saved, grad_out, batch, seq_len, place, to_rel, nat_to_rel):
    w_qkv, w_out, w_gate, w_up, w_down, gain_attn, gain_mlp = weights
    (hidden, inv_attn, normed, q_heads, k_heads, v_heads, probs, heads, mid, inv_mlp, normed_mlp, gate_pre, up_proj, act) = saved
    head_dim = 2 * rope_cos.shape[-1]
    num_heads = 15
    tokens = hidden.shape[0]
    rel_x, rel_y = to_rel
    down = scatter_down(act, grad_out, place)
    grad_act = dot(grad_out, w_down, (1, 1))
    gate_sig = jax.nn.sigmoid(gate_pre)
    grad_up = (grad_act * gate_pre * gate_sig).astype(BF)
    grad_gate = (grad_act * up_proj * gate_sig * (1.0 + gate_pre * (1.0 - gate_sig))).astype(BF)
    gate = scatter_wide(mm(normed_mlp, rel_x).astype(BF), grad_gate, XAX, YAX)
    up = scatter_wide(mm(normed_mlp, rel_y).astype(BF), grad_up, YAX, XAX)
    from_gate = dot(grad_gate, w_gate, (1, 1))
    grad_normed_mlp = from_gate + dot(grad_up, w_up, (1, 1))
    grad_mid_norm, grad_gain_mlp = rms_backward(mid, inv_mlp, gain_mlp, grad_normed_mlp)
    grad_mid = grad_out.astype(F32) + grad_mid_norm
    grad_mid_bf = grad_mid.astype(BF)
    out = scatter_wide(mm(heads, nat_to_rel).astype(BF), grad_mid_bf, YAX, XAX)
    grad_attn = dot(grad_mid_bf, w_out, (1, 1)).astype(BF).reshape(batch, seq_len, 5, 3, head_dim)
    grad_v = jnp.einsum("bkgqs,bqkgd->bskd", probs, grad_attn, preferred_element_type=F32)
    grad_v = grad_v.astype(BF).reshape(tokens, -1)
    grad_probs = jnp.einsum("bqkgd,bskd->bkgqs", grad_attn, v_heads, preferred_element_type=F32)
    probs32 = probs.astype(F32)
    grad_scores = probs32 * (grad_probs - jnp.sum(probs32 * grad_probs, axis=-1, keepdims=True)) * head_dim ** -0.5
    grad_scores = grad_scores.astype(BF)
    grad_q = jnp.einsum("bkgqs,bskd->bqkgd", grad_scores, k_heads, preferred_element_type=F32)
    grad_q = rotary(grad_q.reshape(batch, seq_len, num_heads, head_dim), rope_cos, rope_sin, -1.0)
    grad_q = grad_q.astype(BF).reshape(tokens, -1)
    grad_k = jnp.einsum("bkgqs,bqkgd->bskd", grad_scores, q_heads, preferred_element_type=F32)
    grad_k = rotary(grad_k, rope_cos, rope_sin, -1.0).astype(BF).reshape(tokens, -1)
    grad_qkv = jnp.concatenate([grad_q, grad_k, grad_v, jnp.zeros((tokens, QKV_PAD - QKV), BF)], axis=1)
    grad_normed = dot(grad_qkv, w_qkv, (1, 1))
    grad_hidden_norm, grad_gain_attn = rms_backward(hidden, inv_attn, gain_attn, grad_normed)
    grad_hidden = (grad_mid + grad_hidden_norm).astype(BF)
    gains = jnp.stack([grad_gain_attn, grad_gain_mlp])
    gain_rows = lax.dot_general(rel_y.astype(F32), gains, (((0,), (1,)), ((), ())), precision=lax.Precision.HIGHEST, preferred_element_type=F32)
    extra = jnp.pad(gain_rows, ((0, 0), (QKV, QKV_PAD - QKV - 2)))
    qkv = scatter_wide(mm(normed, rel_y).astype(BF), grad_qkv, YAX, XAX, extra)
    down = scatter_z(down)
    mlp = scatter_z(jnp.concatenate([gate, up], axis=1))
    attn = scatter_z(jnp.concatenate([qkv, out], axis=1))
    return grad_hidden, (attn[:, :QKV_PAD], attn[:, QKV_PAD:], mlp[:, :2560], mlp[:, 2560:], down)


def gather_kernel(*refs):
    count = (len(refs) - 3) // 2
    shards, wholes = refs[:count], refs[count:2 * count]
    send_sem, recv_sem, own_sem = refs[2 * count:]
    me = lax.axis_index("fsdp")
    core, x_at, y_at, z_at = me % 2, me // 2 % 2, me // 4 % 2, me // 8
    core_peer = me + 1 - 2 * core
    x_peer = me + 2 - 4 * x_at
    y_peer = me + 4 - 8 * y_at
    z_near = me + 8 - 16 * (z_at % 2)
    z_far = me + 16 - 32 * (z_at // 2)
    far_at = z_at + 2 - 4 * (z_at // 2)
    barrier = pltpu.get_barrier_semaphore()
    for peer in (core_peer, x_peer, y_peer, z_near, z_far):
        pl.semaphore_signal(barrier, inc=1, device_id=(peer,), device_id_type=pl.DeviceIdType.MESH)
    pl.semaphore_wait(barrier, 5)

    def copy(index, stage, source, target, peer):
        return pltpu.make_async_remote_copy(src_ref=source, dst_ref=target, send_sem=send_sem.at[index, stage], recv_sem=recv_sem.at[index, stage],
                                            device_id=(peer,), device_id_type=pl.DeviceIdType.MESH)

    def to_near(index):
        return copy(index, 0, shards[index], wholes[index].at[core, x_at, y_at, z_at], z_near)

    def to_far(index):
        return copy(index, 1, shards[index], wholes[index].at[core, x_at, y_at, z_at], z_far)

    def onward(index):
        part = wholes[index].at[core, x_at, y_at, far_at]
        return copy(index, 2, part, part, z_near)

    def second(index):
        part = wholes[index].at[core, x_at, y_at]
        return copy(index, 3, part, part, y_peer if index % 5 in (2, 4) else x_peer)

    def third(index):
        if index % 5 in (2, 4):
            part = wholes[index].at[core, x_at]
            return copy(index, 4, part, part, x_peer)
        part = wholes[index].at[core, :, y_at]
        return copy(index, 4, part, part, y_peer)

    def last(index):
        part = wholes[index].at[core]
        return copy(index, 5, part, part, core_peer)

    def own(index):
        return pltpu.make_async_copy(shards[index], wholes[index].at[core, x_at, y_at, z_at], own_sem.at[index])

    def begin(index):
        if index < count:
            own(index).start()
            to_far(index).start()
            to_near(index).start()

    for index in range(3):
        begin(index)
    for turn in range(count + 6):
        begin(turn + 3)
        if turn < count:
            to_far(turn).wait()
            onward(turn).start()
        if 0 <= turn - 1 < count:
            own(turn - 1).wait()
            to_near(turn - 1).wait()
            onward(turn - 1).wait()
            second(turn - 1).start()
        if 0 <= turn - 3 < count:
            second(turn - 3).wait()
            third(turn - 3).start()
        if 0 <= turn - 6 < count:
            third(turn - 6).wait()
            last(turn - 6).start()
    for index in range(count):
        last(index).wait()


def gather_all(shards):
    count = len(shards)
    wholes = pl.pallas_call(
        gather_kernel,
        out_shape=[jax.ShapeDtypeStruct((2, 2, 2, 4) + shard.shape, BF) for shard in shards],
        in_specs=[pl.BlockSpec(memory_space=pltpu.VMEM)] * count,
        out_specs=[pl.BlockSpec(memory_space=pl.ANY)] * count,
        scratch_shapes=[pltpu.SemaphoreType.DMA((count, 6)), pltpu.SemaphoreType.DMA((count, 6)), pltpu.SemaphoreType.DMA((count,))],
        compiler_params=pltpu.CompilerParams(collective_id=0, has_side_effects=True, vmem_limit_bytes=8 * 1024 * 1024),
    )(*shards)
    return [whole.reshape(DEVICES * whole.shape[4], whole.shape[5]) for whole in wholes]


def solution(mesh):
    shard_spec = P(None, "fsdp")
    batch_spec = P("fsdp")

    def local_step(w_query, w_key, w_value, w_out, w_gate, w_up, w_down, gain_attn, gain_mlp, rope_cos, rope_sin, x_in, y_cot):
        me = lax.axis_index("fsdp")
        place = (me % 2, me // 2 % 2, me // 4 % 2, me // 8)
        my_block = block_of(me)
        batch, seq_len, _ = x_in.shape
        tokens = batch * seq_len
        natural = lax.iota(jnp.int32, DIM)
        nat_block, nat_row = block_of(natural // ROWS), natural % ROWS
        spread = one_hot(nat_block * PAD_ROWS + nat_row, PAD_DIM)
        nat_to_rel = one_hot(swap_xy(nat_block ^ my_block) * PAD_ROWS + nat_row, PAD_DIM)
        padded = lax.iota(jnp.int32, PAD_DIM)
        rel_block = (padded // PAD_ROWS) ^ my_block
        rel_x = one_hot(rel_block * PAD_ROWS + padded % PAD_ROWS, PAD_DIM)
        rel_y = one_hot(swap_xy(rel_block) * PAD_ROWS + padded % PAD_ROWS, PAD_DIM)

        def pad_rows(values):
            return jnp.pad(values, ((0, 0), (0, PAD_ROWS - ROWS), (0, 0)))

        def ffn_columns(values):
            return values.reshape(2, ROWS, 4, 2, 2, 2, FFN_ROWS).transpose(0, 1, 5, 4, 3, 2, 6).reshape(2, ROWS, -1)

        sh_qkv = pad_rows(jnp.concatenate([w_query, w_key, w_value, gain_attn[:, :, None], gain_mlp[:, :, None], jnp.zeros((2, ROWS, QKV_PAD - QKV - 2), F32)], axis=2).astype(BF))
        sh_out = pad_rows(mm(w_out.astype(BF).reshape(2 * ROWS, DIM), spread).astype(BF).reshape(2, ROWS, PAD_DIM))
        sh_gate = pad_rows(ffn_columns(w_gate.astype(BF)))
        sh_up = pad_rows(ffn_columns(w_up.astype(BF)))
        sh_down = mm(w_down.astype(BF).reshape(2 * FFN_ROWS, DIM), spread).astype(BF).reshape(2, FFN_ROWS, PAD_DIM)

        hidden = mm(x_in.reshape(tokens, DIM), spread).astype(BF)
        grad_hidden = mm(y_cot.reshape(tokens, DIM), spread).astype(BF)
        saved_layers, layer_weights = [], []
        wholes = gather_all([part[layer] for layer in range(2) for part in (sh_qkv, sh_out, sh_gate, sh_up, sh_down)])
        for layer in range(2):
            full_qkv, full_out, full_gate, full_up, full_down = wholes[5 * layer:5 * layer + 5]
            full_out = mm(spread, full_out).astype(BF)
            weights = (full_qkv, full_out, full_gate, full_up, full_down, full_qkv[:, QKV], full_qkv[:, QKV + 1])
            hidden, saved = layer_forward(weights, rope_cos, rope_sin, hidden, batch, seq_len)
            saved_layers.append(saved)
            layer_weights.append(weights)
        y_out = dot(hidden, spread, (1, 1)).astype(BF).reshape(x_in.shape)
        shards = [None, None]
        for layer in (1, 0):
            grad_hidden, shards[layer] = layer_backward(layer_weights[layer], rope_cos, rope_sin, saved_layers[layer], grad_hidden, batch, seq_len, place, (rel_x, rel_y), nat_to_rel)
        dx_in = dot(grad_hidden, spread, (1, 1)).astype(BF).reshape(x_in.shape)

        g_qkv, g_out, g_gate, g_up, g_down = (jnp.stack(pair) for pair in zip(*shards))

        def natural_columns(values, rows):
            flat = values.reshape(2 * values.shape[1], PAD_DIM)
            flat = lax.dot_general(flat, spread.astype(F32), (((1,), (1,)), ((), ())), precision=lax.Precision.HIGHEST, preferred_element_type=F32)
            return flat.reshape(2, values.shape[1], DIM)[:, :rows]

        def natural_ffn(values):
            return values[:, :ROWS].reshape(2, ROWS, 2, 2, 2, 4, FFN_ROWS).transpose(0, 1, 5, 4, 3, 2, 6).reshape(2, ROWS, -1)

        g_qkv = g_qkv[:, :ROWS]
        return (y_out, dx_in, g_qkv[:, :, :960], g_qkv[:, :, 960:1280], g_qkv[:, :, 1280:1600], natural_columns(g_out, ROWS),
                natural_ffn(g_gate), natural_ffn(g_up), natural_columns(g_down, FFN_ROWS), g_qkv[:, :, QKV], g_qkv[:, :, QKV + 1])

    in_specs = (shard_spec,) * 9 + (P(), P(), batch_spec, batch_spec)
    out_specs = (batch_spec, batch_spec) + (shard_spec,) * 9
    return jax.shard_map(local_step, mesh=mesh, in_specs=in_specs, out_specs=out_specs, check_vma=False)
```
